16 devices in a mesh: fsdp: 16 (over z, y, x, core).
Axes of the slice: x: 2, y: 2, z: 2, core: 2. Of those that a mesh axis runs over, the one named last changes fastest.
Arguments:
- hidden: bfloat16 [16384, 1152], P('fsdp')
- targets: int32 [16384], P('fsdp')
- resp_mask: int32 [16384], P('fsdp')
- resp_id: int32 [16384], P('fsdp')
- old_logp: float32 [16384], P('fsdp')
- ref_logp: float32 [16384], P('fsdp')
- rewards: float32 [128], P('fsdp')
- prompt_id: int32 [128], P('fsdp')
- norm_w: bfloat16 [1152], P('fsdp')
- embedding: bfloat16 [32000, 1152], P('fsdp')
Outputs:
- output 1: float32 [], replicated
- output 2: bfloat16 [16384, 1152], P('fsdp')
- output 3: float32 [32000, 1152], P('fsdp')
- output 4: float32 [1152], P('fsdp')
All inputs are finite; a program needn't handle non-finite values.
Results may differ from the reference program's by a relative error of at most 0.00129.
Values are sent between devices in bfloat16 or wider.
A program may use at most 1 GiB of HBM per device.

```python
import jax
import jax.numpy as jnp
from jax import lax

NUM_SHARDS = 16
TOKENS_DEV = 1024
RESP_DEV = 8
GROUP_SIZE = 8
MODEL_DIM = 1152
VOCAB_SIZE = 32000

TOKENS_ALL = NUM_SHARDS * TOKENS_DEV
RESP_ALL = NUM_SHARDS * RESP_DEV
PROMPTS = RESP_ALL // GROUP_SIZE
TOK_BLOCK = min(TOKENS_DEV, 256)
CLIP_LOW = 0.8
CLIP_HIGH = 1.28
KL_COEF = 0.04
EPSILON = 1e-6


def norm_parts(hidden, norm_w):
    hid_f32 = hidden.astype(jnp.float32)
    inv_rms = lax.rsqrt(jnp.mean(hid_f32 * hid_f32, axis=-1, keepdims=True) + EPSILON)
    normed = hid_f32 * inv_rms
    x_rows = (normed * norm_w.astype(jnp.float32)).astype(jnp.bfloat16)
    return normed, inv_rms, x_rows


def token_logp(x_rows, targets, embedding):
    x_blocks = x_rows.reshape(-1, TOK_BLOCK, MODEL_DIM)
    tgt_blocks = targets.reshape(-1, TOK_BLOCK)

    def one_block(pair):
        x_block, tgt_block = pair
        logits = jnp.dot(x_block, embedding.T, preferred_element_type=jnp.float32)
        picked = jnp.take_along_axis(logits, tgt_block[:, None], axis=1)[:, 0]
        return picked - jax.nn.logsumexp(logits, axis=-1)

    return lax.map(one_block, (x_blocks, tgt_blocks)).reshape(-1)


def group_adv(rewards, prompt_id):
    rew_stats = jnp.stack([rewards, rewards * rewards, jnp.ones_like(rewards)], axis=1)
    totals = jax.ops.segment_sum(rew_stats, prompt_id, num_segments=PROMPTS)
    mean_r = totals[:, 0] / totals[:, 2]
    std_r = jnp.sqrt(jnp.maximum(totals[:, 1] / totals[:, 2] - mean_r * mean_r, 0.0))
    return (rewards - mean_r[prompt_id]) / (std_r[prompt_id] + EPSILON)


def token_terms(tok_logp, old_block, ref_block, adv_block):
    ratio = jnp.exp(tok_logp - old_block)
    surr_raw = ratio * adv_block
    surr_clip = jnp.clip(ratio, CLIP_LOW, CLIP_HIGH) * adv_block
    kl_gap = ref_block - tok_logp
    tok_loss = -jnp.minimum(surr_raw, surr_clip) + KL_COEF * (jnp.exp(kl_gap) - kl_gap - 1.0)
    keep = (surr_raw <= surr_clip) | ((ratio > CLIP_LOW) & (ratio < CLIP_HIGH))
    d_logp = -jnp.where(keep, surr_raw, 0.0) + KL_COEF * (1.0 - jnp.exp(kl_gap))
    return tok_loss, d_logp


def draw_layout(key):
    k_cut, k_cap, k_len = jax.random.split(key, 3)
    cuts = jnp.sort(jax.random.permutation(k_cut, TOKENS_DEV - 1)[:RESP_DEV - 1] + 1).astype(jnp.int32)
    tok_pos = jnp.arange(TOKENS_DEV, dtype=jnp.int32)
    resp_id = jnp.sum((tok_pos[:, None] >= cuts[None, :]).astype(jnp.int32), axis=1)
    starts = jnp.concatenate([jnp.zeros((1,), jnp.int32), cuts])
    len_cap = jax.random.randint(k_cap, (), 1, 2 * (TOKENS_DEV // RESP_DEV) + 1)
    prompt_len = jax.random.randint(k_len, (RESP_DEV,), 0, len_cap)
    in_resp = (tok_pos - starts[resp_id] >= prompt_len[resp_id]) | (tok_pos == TOKENS_DEV - 1)
    return resp_id, in_resp.astype(jnp.int32)


def draw_shift(key):
    k_kind, k_in, k_low, k_high = jax.random.split(key, 4)
    kind = jax.random.randint(k_kind, (TOKENS_ALL,), 0, 3)
    inside = jax.random.uniform(k_in, (TOKENS_ALL,), jnp.float32, -0.15, 0.15)
    below = jax.random.uniform(k_low, (TOKENS_ALL,), jnp.float32, -0.7, -0.3)
    above = jax.random.uniform(k_high, (TOKENS_ALL,), jnp.float32, 0.32, 0.7)
    return jnp.where(kind == 0, inside, jnp.where(kind == 1, below, above))


def setup_inputs(seed: int = 0) -> dict:
    key_list = jax.random.split(jax.random.key(seed), 9)
    resp_id, resp_mask = jax.vmap(draw_layout)(jax.random.split(key_list[0], NUM_SHARDS))
    prompt_id = (jax.random.permutation(key_list[1], RESP_ALL) // GROUP_SIZE).astype(jnp.int32)
    targets = jax.random.randint(key_list[2], (TOKENS_ALL,), 0, VOCAB_SIZE, dtype=jnp.int32)
    hidden = jax.random.normal(key_list[3], (TOKENS_ALL, MODEL_DIM), jnp.float32).astype(jnp.bfloat16)
    norm_w = (1.0 + 0.3 * jax.random.normal(key_list[4], (MODEL_DIM,), jnp.float32)).astype(jnp.bfloat16)
    embedding = (jax.random.normal(key_list[5], (VOCAB_SIZE, MODEL_DIM), jnp.float32) * MODEL_DIM ** -0.5).astype(jnp.bfloat16)
    rewards = jax.random.normal(key_list[6], (RESP_ALL,), jnp.float32)
    base_logp = token_logp(norm_parts(hidden, norm_w)[2], targets, embedding)
    old_logp = base_logp - draw_shift(key_list[7])
    ref_logp = base_logp + jax.random.uniform(key_list[8], (TOKENS_ALL,), jnp.float32, -2.5, 2.5)
    return {'hidden': hidden, 'targets': targets, 'resp_mask': resp_mask.reshape(-1), 'resp_id': resp_id.reshape(-1), 'old_logp': old_logp, 'ref_logp': ref_logp, 'rewards': rewards, 'prompt_id': prompt_id, 'norm_w': norm_w, 'embedding': embedding}


def reference(hidden, targets, resp_mask, resp_id, old_logp, ref_logp, rewards, prompt_id, norm_w, embedding):
    adv_resp = group_adv(rewards, prompt_id)
    owner = jnp.arange(TOKENS_ALL, dtype=jnp.int32) // TOKENS_DEV
    adv_tok = adv_resp[owner * RESP_DEV + resp_id]
    mask_f = resp_mask.astype(jnp.float32)
    count = jnp.sum(mask_f)
    normed, inv_rms, x_rows = norm_parts(hidden, norm_w)
    n_blocks = TOKENS_ALL // TOK_BLOCK
    vocab_ids = jnp.arange(VOCAB_SIZE, dtype=jnp.int32)

    def step(grad_emb, pack):
        x_block, tgt_block, mask_block, old_block, ref_block, adv_block = pack
        logits = jnp.dot(x_block, embedding.T, preferred_element_type=jnp.float32)
        log_norm = jax.nn.logsumexp(logits, axis=-1)
        tok_logp = jnp.take_along_axis(logits, tgt_block[:, None], axis=1)[:, 0] - log_norm
        tok_loss, d_logp = token_terms(tok_logp, old_block, ref_block, adv_block)
        tok_coef = mask_block * d_logp / count
        probs = jnp.exp(logits - log_norm[:, None])
        onehot = (vocab_ids[None, :] == tgt_block[:, None]).astype(jnp.float32)
        d_logits = (tok_coef[:, None] * (onehot - probs)).astype(jnp.bfloat16)
        dx_block = jnp.dot(d_logits, embedding, preferred_element_type=jnp.float32)
        grad_emb = grad_emb + jnp.dot(d_logits.T, x_block, preferred_element_type=jnp.float32)
        return grad_emb, (jnp.sum(mask_block * tok_loss), dx_block)

    pack = (x_rows.reshape(n_blocks, TOK_BLOCK, MODEL_DIM), targets.reshape(n_blocks, TOK_BLOCK), mask_f.reshape(n_blocks, TOK_BLOCK), old_logp.reshape(n_blocks, TOK_BLOCK), ref_logp.reshape(n_blocks, TOK_BLOCK), adv_tok.reshape(n_blocks, TOK_BLOCK))
    init_grad = jnp.zeros((VOCAB_SIZE, MODEL_DIM), jnp.float32)
    d_embedding, (loss_parts, dx_blocks) = lax.scan(step, init_grad, pack)
    d_x = dx_blocks.reshape(TOKENS_ALL, MODEL_DIM)
    d_norm_w = jnp.sum(d_x * normed, axis=0)
    d_normed = d_x * norm_w.astype(jnp.float32)
    d_hidden = (inv_rms * (d_normed - normed * jnp.mean(d_normed * normed, axis=-1, keepdims=True))).astype(jnp.bfloat16)
    mean_loss = jnp.sum(loss_parts) / count
    return mean_loss, d_hidden, d_embedding, d_norm_w
```

```python
import functools

import jax
import jax.numpy as jnp
from jax import lax
from jax.experimental import pallas as pl
from jax.experimental.pallas import tpu as pltpu
from jax.sharding import PartitionSpec as P


GROUP_SIZE = 8
CLIP_LOW = 0.8
CLIP_HIGH = 1.28
KL_COEF = 0.04
EPSILON = 1e-6
CHUNKS = 4
GROUP = 2
BF16 = jnp.bfloat16
F32 = jnp.float32
RELATIVE = (0, 2, 4, 6, 1, 3, 5, 7)
PARAMS = pltpu.CompilerParams(vmem_limit_bytes=62 * 1024 * 1024)
ANY = pl.BlockSpec(memory_space=pl.ANY)
LIST = 32
SLOTS = 2
BOTH_LAST = (((1,), (1,)), ((), ()))
PIECE = 256
N_LISTS = 11
ACTIVE = N_LISTS * LIST
COUNTS = ACTIVE + LIST
PLACE = COUNTS + N_LISTS
FIRST = PLACE + 8


def token_terms(tok_logp, old_block, ref_block, adv_block):
    ratio = jnp.exp(tok_logp - old_block)
    surr_raw = ratio * adv_block
    surr_clip = jnp.clip(ratio, CLIP_LOW, CLIP_HIGH) * adv_block
    kl_gap = ref_block - tok_logp
    tok_loss = -jnp.minimum(surr_raw, surr_clip) + KL_COEF * (jnp.exp(kl_gap) - kl_gap - 1.0)
    keep = (surr_raw <= surr_clip) | ((ratio > CLIP_LOW) & (ratio < CLIP_HIGH))
    d_logp = -jnp.where(keep, surr_raw, 0.0) + KL_COEF * (1.0 - jnp.exp(kl_gap))
    return tok_loss, d_logp


def corner(*_):
    return 0, 0


def row_ids(cols):
    return lax.broadcasted_iota(jnp.int32, (8, cols), 0)


def logits_call(tab, which, emb, x_all, tgt, prev, order, row, first_block, blocks, wide, hid=None, gain8=None):
    rows, dim = emb.shape
    total = tgt.shape[1]
    make = hid is not None
    at = lambda i, t: t[row * LIST + i]

    def body(tab_ref, emb_ref, tgt_ref, src_ref, *refs):
        z_ref, stat_ref = refs[-2:]

        @pl.when(pl.program_id(0) < tab_ref[COUNTS + row])
        def _():
            x_ref = src_ref
            if make:
                x_ref = refs[-3]
                gain = refs[0][pl.ds(0, 1), :]
                for r in range(0, wide, 32):
                    hid = src_ref[pl.ds(r, 32), :].astype(F32)
                    inv = lax.rsqrt(jnp.mean(hid * hid, axis=-1, keepdims=True) + EPSILON)
                    x_ref[pl.ds(r, 32), :] = (hid * inv * gain).astype(BF16)
            rel = tgt_ref[pl.ds(0, 1), :] - tab_ref[FIRST + which]
            ids = row_ids(wide)
            tops, tots, hits = [], [], []
            for a in range(0, rows, 400):
                sub = 400
                z_ref[pl.ds(a, sub), :] = lax.dot_general(emb_ref[pl.ds(a, sub), :], x_ref[...], BOTH_LAST, preferred_element_type=F32)
                top = z_ref[pl.ds(a, 8), :]
                for r in range(a, a + sub, 8):
                    top = jnp.maximum(top, z_ref[pl.ds(r, 8), :])
                tot = jnp.zeros((8, wide), F32)
                hit = jnp.zeros((8, wide), F32)
                for r in range(a, a + sub, 8):
                    z = z_ref[pl.ds(r, 8), :]
                    tot = tot + jnp.exp(z - top)
                    hit = hit + jnp.where(ids == rel - r, z, 0.0)
                tops.append(top)
                tots.append(tot)
                hits.append(hit)
            top = jnp.max(functools.reduce(jnp.maximum, tops), axis=0, keepdims=True)
            tot = sum(t * jnp.exp(m - top) for m, t in zip(tops, tots))
            down = lambda v: jnp.sum(v, axis=0, keepdims=True)
            stat_ref[...] = jnp.concatenate([top, down(tot), down(sum(hits)), jnp.zeros((5, wide), F32)], axis=0)

    in_specs = [
        pl.BlockSpec((rows, dim), corner, pipeline_mode=pl.Buffered(1)),
        pl.BlockSpec((8, wide), lambda i, t: (0, at(i, t))),
        pl.BlockSpec((wide, dim), lambda i, t: ((t[PLACE + at(i, t) - first_block] if make else at(i, t)), 0)),
    ]
    args = [tab, emb, tgt, hid if make else x_all]
    out_shape = [jax.ShapeDtypeStruct((rows, total), F32), jax.ShapeDtypeStruct((8, blocks * wide), F32)]
    out_specs = [pl.BlockSpec((rows, wide), lambda i, t: (0, at(i, t))), pl.BlockSpec((8, wide), lambda i, t: (0, at(i, t) - first_block))]
    if make:
        in_specs.append(pl.BlockSpec((8, dim), corner))
        args.append(gain8)
        out_shape.insert(0, jax.ShapeDtypeStruct((total, dim), BF16))
        out_specs.insert(0, pl.BlockSpec((wide, dim), lambda i, t: (at(i, t), 0)))
    in_specs.append(ANY)
    args.append(order)
    alias = {len(args) + j: j for j in range(len(prev))}
    return pl.pallas_call(
        body,
        out_shape=out_shape,
        grid_spec=pltpu.PrefetchScalarGridSpec(num_scalar_prefetch=1, grid=(blocks,), in_specs=in_specs + [ANY] * len(prev), out_specs=out_specs),
        input_output_aliases=alias,
        compiler_params=PARAMS,
        name='logits',
    )(*args, *prev)


def grad_rows(z_ref, out_ref, base, col, a, n, meta, rel):
    lse, coef = meta[0:1], meta[1:2]
    wide = meta.shape[1]
    ids = row_ids(wide)
    for r in range(a, a + n, 8):
        prob = jnp.exp(z_ref[pl.ds(r, 8), :] - lse)
        grad = coef * (jnp.where(ids == rel - r, 1.0, 0.0) - prob)
        out_ref[pl.ds(base + r, 8), pl.ds(col, wide)] = grad.astype(BF16)


def dx_call(tab, z_own, z_par, turned_own, turned_par, meta, order, row, first_block, blocks, wide, begin=None):
    rows, _ = z_own.shape
    dim, padded = turned_own.shape
    half = dim // 2
    sub = 256
    keep = begin is not None
    at = lambda i, t: t[row * LIST + i]

    def body(tab_ref, zo_ref, zp_ref, eto_ref, etp_ref, meta_ref, *refs):
        dz_ref, acc_ref = refs[-2:]
        step = pl.program_id(0)
        place = step % 4
        block = first_block + (step // 4) * 8 + place

        @pl.when(tab_ref[ACTIVE + block] > 0)
        def _():
            meta = meta_ref[...]
            tgt = meta[2:3].astype(jnp.int32)
            for h, (z_ref, et_ref) in enumerate(((zo_ref, eto_ref), (zp_ref, etp_ref))):
                dz_ref[pl.ds(h * padded + rows, padded - rows), :] = jnp.zeros((padded - rows, wide), BF16)
                for a in range(0, padded, sub):
                    grad_rows(z_ref, dz_ref, h * padded, 0, a, min(sub, rows - a), meta, tgt - tab_ref[FIRST + h])
                    part = jnp.dot(et_ref[:, pl.ds(a, sub)], dz_ref[pl.ds(h * padded + a, sub), :], preferred_element_type=F32)
                    acc_ref[...] = part if h + a == 0 else acc_ref[...] + part

        @pl.when(tab_ref[ACTIVE + block] == 0)
        def _():
            acc_ref[...] = jnp.zeros_like(acc_ref)

        if not keep:
            refs[1][0] = acc_ref[...]
            return
        start_ref, keep_a, send_a, keep_b, send_b = refs[1:6]
        for q in range(4):

            @pl.when(place == q)
            def _():
                (send_a if q % 2 else keep_a)[0] = acc_ref[pl.ds(0, half), :] + start_ref[0, pl.ds(0, half), :]
                (send_b if q // 2 else keep_b)[q % 2] = acc_ref[pl.ds(half, half), :] + start_ref[0, pl.ds(half, half), :]

    in_specs = [
        pl.BlockSpec((rows, wide), lambda i, t: (0, at(i, t))),
        pl.BlockSpec((rows, wide), lambda i, t: (0, at(i, t))),
        pl.BlockSpec((dim, padded), corner, pipeline_mode=pl.Buffered(1)),
        pl.BlockSpec((dim, padded), corner, pipeline_mode=pl.Buffered(1)),
        pl.BlockSpec((8, wide), lambda i, t: (0, at(i, t))),
        ANY,
    ]
    args = [tab, z_own, z_par, turned_own, turned_par, meta, order]
    one = pl.BlockSpec((1, dim, wide), lambda i, t: (i, 0, 0))
    if keep:
        in_specs.append(one)
        args.append(begin)
        out_shape = [jax.ShapeDtypeStruct((blocks // 2, half, wide), F32)] * 4
        by_place = pl.BlockSpec((1, half, wide), lambda i, t: (i // 2, 0, 0))
        by_chunk = pl.BlockSpec((2, half, wide), lambda i, t: (i // 4, 0, 0))
        out_specs = [by_place, by_place, by_chunk, by_chunk]
    else:
        out_shape = jax.ShapeDtypeStruct((blocks, dim, wide), F32)
        out_specs = one
    return pl.pallas_call(
        body,
        out_shape=out_shape,
        grid_spec=pltpu.PrefetchScalarGridSpec(
            num_scalar_prefetch=1,
            grid=(blocks,),
            in_specs=in_specs,
            out_specs=out_specs,
            scratch_shapes=[pltpu.VMEM((2 * padded, wide), BF16), pltpu.VMEM((dim, wide), F32)],
        ),
        compiler_params=PARAMS,
        name='dx',
    )(*args)


def de_call(tab, which, z, x_all, meta, order, row, part, n_parts, wide, begin=None, into=None):
    rows_all, total = z.shape
    rows = rows_all // n_parts
    dim = x_all.shape[1]
    at = lambda j: (lambda i, t: t[row * LIST + i * SLOTS + j])

    def body(tab_ref, *refs):
        z_refs, x_refs, meta_refs = refs[:SLOTS], refs[SLOTS:2 * SLOTS], refs[2 * SLOTS:3 * SLOTS]
        out_ref, dz_ref, rows_ref = refs[-3:]
        step = pl.program_id(0)

        @pl.when(step == 0)
        def _():
            out_ref[...] = jnp.zeros_like(out_ref) if begin is None else refs[3 * SLOTS + 1][...]

        @pl.when(step * SLOTS < tab_ref[COUNTS + row])
        def _():
            metas, rels = [], []
            for j in range(SLOTS):
                meta = meta_refs[j][...]
                live = jnp.where(step * SLOTS + j < tab_ref[COUNTS + row], 1.0, 0.0)
                rels.append(meta[2:3].astype(jnp.int32) - tab_ref[FIRST + which] - part * rows)
                metas.append(jnp.concatenate([meta[0:1], meta[1:2] * live], axis=0))
                rows_ref[pl.ds(j * wide, wide), :] = x_refs[j][...]
            for a in range(0, rows, PIECE):
                n = min(PIECE, rows - a)
                for j in range(SLOTS):
                    grad_rows(z_refs[j], dz_ref, 0, j * wide, a, n, metas[j], rels[j])
                out_ref[pl.ds(a, n), :] += jnp.dot(dz_ref[pl.ds(a, n), :], rows_ref[...], preferred_element_type=F32)

    maps = [at(j) for j in range(SLOTS)]
    in_specs = [pl.BlockSpec((rows, wide), lambda i, t, m=m: (part, m(i, t))) for m in maps]
    in_specs += [pl.BlockSpec((wide, dim), lambda i, t, m=m: (m(i, t), 0)) for m in maps]
    in_specs += [pl.BlockSpec((8, wide), lambda i, t, m=m: (0, m(i, t))) for m in maps] + [ANY]
    order = meta if order is into else order
    args = [tab] + [z] * SLOTS + [x_all] * SLOTS + [meta] * SLOTS + [order]
    alias = {}
    whole = begin is not None
    if whole:
        in_specs.append(pl.BlockSpec((rows, dim), corner, pipeline_mode=pl.Buffered(1)))
        args.append(begin)
    if into is not None:
        alias = {len(args): 0}
        in_specs.append(ANY)
        args.append(into)
    return pl.pallas_call(
        body,
        out_shape=jax.ShapeDtypeStruct((rows_all if whole else rows, dim), F32),
        grid_spec=pltpu.PrefetchScalarGridSpec(
            num_scalar_prefetch=1,
            grid=(total // wide // SLOTS,),
            in_specs=in_specs,
            out_specs=pl.BlockSpec((rows, dim), lambda i, t: (part if whole else 0, 0)),
            scratch_shapes=[pltpu.VMEM((rows, SLOTS * wide), BF16), pltpu.VMEM((SLOTS * wide, dim), BF16)],
        ),
        input_output_aliases=alias,
        compiler_params=PARAMS,
        name='de',
    )(*args)


def turn_call(emb, order):
    rows, dim = emb.shape
    n = pl.cdiv(rows, 256)

    def body(emb_ref, order_ref, out_ref):
        left = rows - pl.program_id(0) * 256
        row = lax.broadcasted_iota(jnp.int32, emb_ref.shape, 0)
        out_ref[...] = jnp.where(row < left, emb_ref[...], jnp.zeros_like(emb_ref)).T

    return pl.pallas_call(
        body,
        grid=(n,),
        out_shape=jax.ShapeDtypeStruct((dim, n * 256), BF16),
        in_specs=[pl.BlockSpec((256, dim), lambda i: (i, 0)), ANY],
        out_specs=pl.BlockSpec((dim, 256), lambda i: (0, i)),
        compiler_params=PARAMS,
        name='turn',
    )(emb, order)


def flipped(me, mask):
    out = me
    bit = 1
    while bit <= mask:
        if mask & bit:
            out = out + bit - 2 * bit * ((me // bit) % 2)
        bit *= 2
    return out


def share_call(block, shards, ident):
    def body(in_ref, out_ref, send_sem, recv_sem):
        me = lax.axis_index('fsdp')
        peers = [flipped(me, r) for r in range(1, shards)]
        barrier = pltpu.get_barrier_semaphore()
        for peer in peers:
            pl.semaphore_signal(barrier, inc=1, device_id=(peer,), device_id_type=pl.DeviceIdType.MESH)
        pl.semaphore_wait(barrier, shards - 1)
        copies = []
        for r, peer in enumerate(peers):
            copy = pltpu.make_async_remote_copy(src_ref=in_ref, dst_ref=out_ref.at[me], send_sem=send_sem.at[r], recv_sem=recv_sem.at[r], device_id=(peer,), device_id_type=pl.DeviceIdType.MESH)
            copy.start()
            copies.append(copy)
        out_ref[me] = in_ref[...]
        for copy in copies:
            copy.wait()

    return pl.pallas_call(
        body,
        out_shape=jax.ShapeDtypeStruct((shards,) + block.shape, block.dtype),
        in_specs=[pl.BlockSpec(memory_space=pltpu.VMEM)],
        out_specs=pl.BlockSpec(memory_space=pltpu.VMEM),
        scratch_shapes=[pltpu.SemaphoreType.DMA((shards - 1,)), pltpu.SemaphoreType.DMA((shards - 1,))],
        compiler_params=pltpu.CompilerParams(collective_id=ident, has_side_effects=True),
        name='share',
    )(block)


def coef_call(own_stats, par_stats, token, tgt, team, wide, ident):
    tok_dev = token.shape[1]
    n = tok_dev // wide
    n_own, n_par = len(own_stats), len(par_stats)

    def body(*refs):
        own, par = refs[:n_own], refs[n_own:n_own + n_par]
        token_ref, tgt_ref, meta_ref, loss_ref, out_buf, in_buf, send2, back, send_sem, recv_sem, send_sem2, recv_sem2 = refs[n_own + n_par:]
        me = lax.axis_index('fsdp')
        peers = [flipped(me, r) for r in RELATIVE[1:]]
        for ref in (out_buf, send2, meta_ref):
            ref[...] = jnp.zeros_like(ref)
        for k in range(n):
            a = own[k * n_own // n][:, pl.ds(k % (n // n_own) * team * wide, team * wide)]
            b = par[k * n_par // n][:, pl.ds(k % (n // n_par) * team * wide, team * wide)]
            top = jnp.maximum(a[0:1], b[0:1])
            tot = a[1:2] * jnp.exp(a[0:1] - top) + b[1:2] * jnp.exp(b[0:1] - top)
            hit = a[2:3] + b[2:3]
            for p in range(team):
                at = slice(p * wide, (p + 1) * wide)
                dst = out_buf if p else in_buf
                dst[p, 0:1, pl.ds(k * wide, wide)] = top[:, at]
                dst[p, 1:2, pl.ds(k * wide, wide)] = tot[:, at]
                dst[p, 2:3, pl.ds(k * wide, wide)] = hit[:, at]
        barrier = pltpu.get_barrier_semaphore()
        for peer in peers:
            pl.semaphore_signal(barrier, inc=1, device_id=(peer,), device_id_type=pl.DeviceIdType.MESH)
        pl.semaphore_wait(barrier, team - 1)
        copies = []
        for p in range(1, team):
            copy = pltpu.make_async_remote_copy(src_ref=out_buf.at[p], dst_ref=in_buf.at[p], send_sem=send_sem.at[p], recv_sem=recv_sem.at[p], device_id=(peers[p - 1],), device_id_type=pl.DeviceIdType.MESH)
            copy.start()
            copies.append(copy)
        for copy in copies:
            copy.wait()
        top = in_buf[0, 0:1, :]
        for p in range(1, team):
            top = jnp.maximum(top, in_buf[p, 0:1, :])
        tot = jnp.zeros_like(top)
        hit = jnp.zeros_like(top)
        for p in range(team):
            tot = tot + in_buf[p, 1:2, :] * jnp.exp(in_buf[p, 0:1, :] - top)
            hit = hit + in_buf[p, 2:3, :]
        lse = top + jnp.log(tot)
        mask = token_ref[0:1, :]
        tok_loss, d_logp = token_terms(hit - lse, token_ref[1:2, :], token_ref[2:3, :], token_ref[3:4, :])
        send2[0:1, :] = lse
        send2[1:2, :] = jnp.where(mask > 0.0, d_logp / token_ref[4:5, :], 0.0)
        loss_ref[...] = jnp.broadcast_to(jnp.where(mask > 0.0, tok_loss, 0.0), loss_ref.shape)
        copies = []
        for p in range(1, team):
            copy = pltpu.make_async_remote_copy(src_ref=send2, dst_ref=back.at[p], send_sem=send_sem2.at[p], recv_sem=recv_sem2.at[p], device_id=(peers[p - 1],), device_id_type=pl.DeviceIdType.MESH)
            copy.start()
            copies.append(copy)
        back[0] = send2[...]
        for copy in copies:
            copy.wait()
        for k in range(n):
            for p in range(team):
                at = pl.ds((k * team + p) * wide, wide)
                meta_ref[0:2, at] = back[p, 0:2, pl.ds(k * wide, wide)]
        meta_ref[2:3, :] = tgt_ref[0:1, :].astype(F32)

    vmem = pl.BlockSpec(memory_space=pltpu.VMEM)
    return pl.pallas_call(
        body,
        out_shape=[jax.ShapeDtypeStruct((8, n * team * wide), F32), jax.ShapeDtypeStruct((8, tok_dev), F32)],
        in_specs=[vmem] * (n_own + n_par + 2),
        out_specs=[vmem, vmem],
        scratch_shapes=[pltpu.VMEM((team, 8, tok_dev), F32), pltpu.VMEM((team, 8, tok_dev), F32), pltpu.VMEM((8, tok_dev), F32), pltpu.VMEM((team, 8, tok_dev), F32)] + [pltpu.SemaphoreType.DMA((team,))] * 4,
        compiler_params=pltpu.CompilerParams(collective_id=ident, has_side_effects=True),
        name='coef',
    )(*own_stats, *par_stats, token, tgt)


def second_sum(keep_a, recv_a, keep_b, recv_b, order):
    n, half, wide = keep_a.shape

    def body(ka, ra, kb, rb, order_ref, fa, sa, fb, sb):
        fa[0] = ka[0] + ra[0]
        sa[0] = ka[1] + ra[1]
        fb[0] = kb[0] + rb[0]
        sb[0] = kb[1] + rb[1]

    step = half // 2
    two = pl.BlockSpec((2, step, wide), lambda g, i: (g, i, 0))
    one = pl.BlockSpec((1, step, wide), lambda g, i: (g, i, 0))
    return pl.pallas_call(
        body,
        grid=(n // 2, 2),
        out_shape=[jax.ShapeDtypeStruct((n // 2, half, wide), F32)] * 4,
        in_specs=[two] * 4 + [ANY],
        out_specs=[one] * 4,
        compiler_params=PARAMS,
        name='second_sum',
    )(keep_a, recv_a, keep_b, recv_b, order)


def hidden_kernel(fa_ref, ra_ref, fb_ref, rb_ref, hid_ref, gain_ref, dg_ref):
    d_x = jnp.concatenate([(fa_ref[0] + ra_ref[0]).T, (fb_ref[0] + rb_ref[0]).T], axis=1)
    hid = hid_ref[...].astype(F32)
    inv = lax.rsqrt(jnp.mean(hid * hid, axis=-1, keepdims=True) + EPSILON)
    normed = hid * inv
    dg_ref[...] = jnp.broadcast_to(jnp.sum(d_x * normed, axis=0, keepdims=True), dg_ref.shape)
    d_normed = d_x * gain_ref[0:1, :]
    return (inv * (d_normed - normed * jnp.mean(d_normed * normed, axis=-1, keepdims=True))).astype(BF16)


def hidden_call(parts, hidden, gain8, to_spot, prev, order, k):
    n, half, wide = parts[0].shape
    tokens, dim = hidden.shape

    def body(*refs):
        spot_ref, dh_ref, dg_ref, acc_ref = refs[6], *refs[-3:]
        step = pl.program_id(0)
        rows = hidden_kernel(*refs[:6], dg_ref)
        back = lax.dot_general(spot_ref[...], rows, (((0,), (0,)), ((), ())), preferred_element_type=F32)

        @pl.when(step == 0)
        def _():
            acc_ref[...] = back if prev is None else back + refs[-4][...].astype(F32)

        @pl.when(step > 0)
        def _():
            dh_ref[...] = (acc_ref[...] + back).astype(BF16)

    in_specs = [pl.BlockSpec((1, half, wide), lambda i: (i, 0, 0))] * 4 + [
        pl.BlockSpec((wide, dim), lambda i: (k * n + i, 0)),
        pl.BlockSpec((8, dim), corner),
        pl.BlockSpec((wide, tokens), lambda i: (k * n + i, 0)),
        ANY,
    ]
    args = [*parts, hidden, gain8, to_spot, order]
    if prev is not None:
        in_specs.append(pl.BlockSpec((tokens, dim), corner))
        args.append(prev)
    return pl.pallas_call(
        body,
        grid=(n,),
        out_shape=[jax.ShapeDtypeStruct(hidden.shape, BF16), jax.ShapeDtypeStruct((8 * n, dim), F32)],
        in_specs=in_specs,
        out_specs=[pl.BlockSpec((tokens, dim), corner), pl.BlockSpec((8, dim), lambda i: (i, 0))],
        scratch_shapes=[pltpu.VMEM((tokens, dim), F32)],
        compiler_params=PARAMS,
        name='hidden',
    )(*args)


PLAN = (
    ('de_par', 0), ('dx_send', 0), ('dx_send', 1), ('dx_keep', 0), ('de_par', 1), ('dx_keep', 1),
    ('sum_two', 0), ('de_own', 0), ('sum_two', 1), ('de_own', 1), ('finish', 0), ('finish', 1),
)


def block_lists():
    span = lambda a, n: list(range(a, a + n))
    team = len(RELATIVE)
    halves = lambda b: [sum((span((g * GROUP + k) * team + b, team // 2) for k in range(GROUP)), []) for g in range(CHUNKS // GROUP)]
    lists = [span(k * team, team) for k in range(CHUNKS)]
    lists += [span(g * GROUP * team, GROUP * team) for g in range(CHUNKS // GROUP)]
    return lists + [span(0, CHUNKS * team)] + halves(team // 2) + halves(0)


def solution(mesh):
    shards = mesh.shape['fsdp']
    team = shards // 2
    teams = [list(range(team)), list(range(team, shards))]

    def local(hidden, targets, resp_mask, resp_id, old_logp, ref_logp, rewards, prompt_id, norm_w, embedding):
        tok_dev, dim = hidden.shape
        rows = embedding.shape[0]
        prompts = rewards.shape[0] * shards // GROUP_SIZE
        resp = rewards.shape[0]
        me = lax.axis_index('fsdp')
        wide = tok_dev // CHUNKS
        total = team * tok_dev

        def trade(value, bit):
            return lax.ppermute(value, 'fsdp', [(i, i ^ bit) for i in range(shards)])

        mask_f = resp_mask.astype(F32)
        spots = jnp.arange(tok_dev, dtype=jnp.int32)
        before = jnp.cumsum(resp_mask)
        spot = jnp.where(resp_mask > 0, before - 1, before[-1] + spots - before)
        to_spot = (spots[:, None] == spot[None, :]).astype(BF16)
        rows_first = jnp.dot(to_spot, hidden, preferred_element_type=F32).astype(BF16)
        hid_chunks = [lax.all_gather(rows_first[k * wide:(k + 1) * wide], 'fsdp', axis_index_groups=teams, tiled=True) for k in range(CHUNKS)]

        raw = jnp.stack([targets.astype(F32), mask_f, old_logp, ref_logp, resp_id.astype(F32)])
        raw = lax.dot_general(raw, to_spot.astype(F32), BOTH_LAST, precision=lax.Precision.HIGHEST)
        lanes = lambda v: jnp.pad(v, (0, -v.size % 128)).reshape(-1, 128)
        few = jnp.concatenate([rewards, prompt_id.astype(F32), jnp.sum(mask_f)[None]])
        small = jnp.concatenate([lanes(raw[0]), lanes(few), lanes(norm_w.astype(F32))])
        small = jnp.pad(small, ((0, -small.shape[0] % 8), (0, 0)))
        every = share_call(small, shards, 1)
        emb_later, every = lax.optimization_barrier((embedding, every))
        emb_par = trade(emb_later, team)
        tgt_rows = tok_dev // 128
        rew_all = every[:, tgt_rows, :resp].reshape(-1)
        prompt_all = every[:, tgt_rows, resp:2 * resp].reshape(-1).astype(jnp.int32)
        counts = every[:, tgt_rows, 2 * resp]
        count = jnp.sum(counts)
        gain = every[:, tgt_rows + 1, :norm_w.shape[0]].reshape(-1)
        in_all = (prompt_all[None, :] == jnp.arange(prompts, dtype=jnp.int32)[:, None]).astype(F32)
        totals = jnp.sum(in_all[None] * jnp.stack([rew_all, rew_all * rew_all, jnp.ones_like(rew_all)])[:, None, :], axis=2)
        mean_r = totals[0] / totals[2]
        std_r = jnp.sqrt(jnp.maximum(totals[1] / totals[2] - mean_r * mean_r, 0.0))
        in_own = (prompt_id[None, :] == jnp.arange(prompts, dtype=jnp.int32)[:, None]).astype(F32)
        pick = lambda v: jnp.sum(in_own * v[:, None], axis=0)
        adv_resp = (rewards - pick(mean_r)) / (pick(std_r) + EPSILON)
        adv_tok = jnp.sum(jnp.where(raw[4][None, :] == jnp.arange(resp, dtype=F32)[:, None], adv_resp[:, None], 0.0), axis=0)
        token = jnp.stack([raw[1], raw[2], raw[3], adv_tok, jnp.full_like(mask_f, count)])
        token = jnp.concatenate([token, jnp.zeros((3, tok_dev), F32)])

        in_team = me % team
        place = jnp.bitwise_xor(in_team, jnp.array(RELATIVE, jnp.int32)).astype(jnp.int32)
        tgt_all = every[me - in_team + place, :tgt_rows, :].reshape(team, CHUNKS, wide).transpose(1, 0, 2).reshape(1, total)
        tgt8 = jnp.broadcast_to(tgt_all.astype(jnp.int32), (8, total))
        gain8 = jnp.broadcast_to(gain[None, :], (8, dim))

        active = (counts[me - in_team + place][None, :] > wide * jnp.arange(CHUNKS, dtype=F32)[:, None]).reshape(-1)
        lists = block_lists()
        ids = jnp.array([ids + [0] * (LIST - len(ids)) for ids in lists], jnp.int32)
        used = jnp.array([[1] * len(ids) + [0] * (LIST - len(ids)) for ids in lists], jnp.int32)
        every_id = jnp.arange(LIST, dtype=jnp.int32)
        live = used * jnp.sum((ids[:, :, None] == every_id) * active[None, None, :].astype(jnp.int32), axis=2)
        upto = jnp.sum(live[:, None, :] * (every_id[None, :] <= every_id[:, None]), axis=2)
        n_live = jnp.sum(live, axis=1)
        packed = jnp.minimum(every_id[None, :], n_live[:, None] - 1)
        want = jnp.where(every_id[:N_LISTS, None] < N_LISTS - 4, packed, jnp.maximum(upto - 1, 0))
        chosen = jnp.sum(ids[:, None, :] * live[:, None, :] * (upto[:, None, :] - 1 == want[:, :, None]), axis=2)
        chosen = jnp.where(n_live[:, None] == 0, ids[:, :1], chosen)
        firsts = jnp.stack([me, (me + team) % shards]) * rows
        tab = jnp.concatenate([chosen.reshape(-1), active.astype(jnp.int32), n_live, place, firsts]).astype(jnp.int32)

        stat_own, stat_par, prev, prev_par = [], [], [], []
        order = turned_own = turn_call(embedding, gain8)

        def own(k):
            x_all, z_own, stat = logits_call(tab, 0, embedding, None, tgt8, prev, order, k, k * team, team, wide, hid_chunks[k], gain8)
            prev[:] = [x_all, z_own]
            stat_own.append(stat)
            return stat

        def par(g):
            z, stat = logits_call(tab, 1, emb_par, prev[0], tgt8, prev_par, order, CHUNKS + g, g * GROUP * team, GROUP * team, wide)
            prev_par[:] = [z]
            stat_par.append(stat)
            return stat

        for k in range(CHUNKS - 1):
            order = own(k)
        order = turned_par = turn_call(emb_par, order)
        order = par(0)
        order = own(CHUNKS - 1)
        order = par(1)
        x_all, z_own = prev
        z_par = prev_par[0]
        meta, loss_own = coef_call(stat_own, stat_par, token, tgt8, team, wide, 2)

        state = {}
        order = meta

        def dx_send(k):
            first_block = k * GROUP * team + team // 2
            out = dx_call(tab, z_own, z_par, turned_own, turned_par, meta, order, N_LISTS - 4 + k, first_block, GROUP * team // 2, wide)
            state[k] = trade(out, 1)
            return out

        def dx_keep(k):
            outs = dx_call(tab, z_own, z_par, turned_own, turned_par, meta, order, N_LISTS - 2 + k, k * GROUP * team, GROUP * team // 2, wide, state[k])
            keep_a, send_a, keep_b, send_b = outs
            state[k] = (keep_a, trade(send_a, 2), keep_b, trade(send_b, 4))
            return keep_a

        def sum_two(k):
            fa, sa, fb, sb = second_sum(*state[k], order)
            state[k] = (fa, trade(sa, 4), fb, trade(sb, 2))
            return fa

        def finish(k):
            out, part = hidden_call(state[k], rows_first, gain8, to_spot, state.get('dh'), order, k)
            state['dh'] = out
            state['dg'] = state.get('dg', []) + [part]
            return part

        def de_par(p):
            out = de_call(tab, 1, z_par, x_all, meta, order, CHUNKS + GROUP, p, 2, wide)
            state['ship', p] = trade(out, team)
            return out

        def de_own(p):
            state['de'] = de_call(tab, 0, z_own, x_all, meta, order, CHUNKS + GROUP, p, 2, wide, state['ship', p], state.get('de'))
            return state['de']

        steps = {'de_par': de_par, 'dx_send': dx_send, 'dx_keep': dx_keep, 'sum_two': sum_two, 'de_own': de_own, 'finish': finish}
        for name, arg in PLAN:
            order = steps[name](arg)
        d_hidden = state['dh']
        d_embedding = state['de']
        gain_sum = jnp.sum(jnp.concatenate(state['dg'], axis=0)[::8], axis=0)
        last = jnp.concatenate([gain_sum.reshape(-1, 128), lanes(jnp.sum(loss_own[0])[None])])
        last = jnp.pad(last, ((0, -last.shape[0] % 8), (0, 0)))
        last = jnp.sum(share_call(last, shards, 3), axis=0)
        d_norm_w = lax.dynamic_slice(last.reshape(-1), (me * norm_w.shape[0],), (norm_w.shape[0],))
        mean_loss = last[dim // 128, 0] / count
        return mean_loss, d_hidden, d_embedding, d_norm_w

    tok_spec = P('fsdp')
    row_spec = P('fsdp', None)
    return jax.shard_map(local, mesh=mesh, in_specs=(row_spec, tok_spec, tok_spec, tok_spec, tok_spec, tok_spec, tok_spec, tok_spec, tok_spec, row_spec), out_specs=(P(), row_spec, row_spec, tok_spec), check_vma=False)
```

```python
import functools

import jax
import jax.numpy as jnp
from jax import lax
from jax.experimental import pallas as pl
from jax.experimental.pallas import tpu as pltpu
from jax.sharding import PartitionSpec as P


GROUP_SIZE = 8
CLIP_LOW = 0.8
CLIP_HIGH = 1.28
KL_COEF = 0.04
EPSILON = 1e-6
CHUNKS = 4
GROUP = 2
BF16 = jnp.bfloat16
F32 = jnp.float32
RELATIVE = (0, 2, 4, 6, 1, 3, 5, 7)
PARAMS = pltpu.CompilerParams(vmem_limit_bytes=62 * 1024 * 1024)
ANY = pl.BlockSpec(memory_space=pl.ANY)
LIST = 32
SLOTS = 2
BOTH_LAST = (((1,), (1,)), ((), ()))
PIECE = 256
N_LISTS = 11
ACTIVE = N_LISTS * LIST
COUNTS = ACTIVE + LIST
PLACE = COUNTS + N_LISTS
FIRST = PLACE + 8


def token_terms(tok_logp, old_block, ref_block, adv_block):
    ratio = jnp.exp(tok_logp - old_block)
    surr_raw = ratio * adv_block
    surr_clip = jnp.clip(ratio, CLIP_LOW, CLIP_HIGH) * adv_block
    kl_gap = ref_block - tok_logp
    tok_loss = -jnp.minimum(surr_raw, surr_clip) + KL_COEF * (jnp.exp(kl_gap) - kl_gap - 1.0)
    keep = (surr_raw <= surr_clip) | ((ratio > CLIP_LOW) & (ratio < CLIP_HIGH))
    d_logp = -jnp.where(keep, surr_raw, 0.0) + KL_COEF * (1.0 - jnp.exp(kl_gap))
    return tok_loss, d_logp


def corner(*_):
    return 0, 0


def row_ids(cols):
    return lax.broadcasted_iota(jnp.int32, (8, cols), 0)


def logits_call(tab, which, emb, x_all, tgt, prev, order, row, first_block, blocks, wide, hid=None, gain8=None):
    rows, dim = emb.shape
    total = tgt.shape[1]
    make = hid is not None
    at = lambda i, t: t[row * LIST + i]

    def body(tab_ref, emb_ref, tgt_ref, src_ref, *refs):
        z_ref, stat_ref = refs[-2:]

        @pl.when(pl.program_id(0) < tab_ref[COUNTS + row])
        def _():
            x_ref = src_ref
            if make:
                x_ref = refs[-3]
                gain = refs[0][pl.ds(0, 1), :]
                for r in range(0, wide, 32):
                    hid = src_ref[pl.ds(r, 32), :].astype(F32)
                    inv = lax.rsqrt(jnp.mean(hid * hid, axis=-1, keepdims=True) + EPSILON)
                    x_ref[pl.ds(r, 32), :] = (hid * inv * gain).astype(BF16)
            rel = tgt_ref[pl.ds(0, 1), :] - tab_ref[FIRST + which]
            ids = row_ids(wide)
            tops, tots, hits = [], [], []
            for a in range(0, rows, 400):
                sub = 400
                z_ref[pl.ds(a, sub), :] = lax.dot_general(emb_ref[pl.ds(a, sub), :], x_ref[...], BOTH_LAST, preferred_element_type=F32)
                top = z_ref[pl.ds(a, 8), :]
                for r in range(a, a + sub, 8):
                    top = jnp.maximum(top, z_ref[pl.ds(r, 8), :])
                tot = jnp.zeros((8, wide), F32)
                hit = jnp.zeros((8, wide), F32)
                for r in range(a, a + sub, 8):
                    z = z_ref[pl.ds(r, 8), :]
                    tot = tot + jnp.exp(z - top)
                    hit = hit + jnp.where(ids == rel - r, z, 0.0)
                tops.append(top)
                tots.append(tot)
                hits.append(hit)
            top = jnp.max(functools.reduce(jnp.maximum, tops), axis=0, keepdims=True)
            tot = sum(t * jnp.exp(m - top) for m, t in zip(tops, tots))
            down = lambda v: jnp.sum(v, axis=0, keepdims=True)
            stat_ref[...] = jnp.concatenate([top, down(tot), down(sum(hits)), jnp.zeros((5, wide), F32)], axis=0)

    in_specs = [
        pl.BlockSpec((rows, dim), corner, pipeline_mode=pl.Buffered(1)),
        pl.BlockSpec((8, wide), lambda i, t: (0, at(i, t))),
        pl.BlockSpec((wide, dim), lambda i, t: ((t[PLACE + at(i, t) - first_block] if make else at(i, t)), 0)),
    ]
    args = [tab, emb, tgt, hid if make else x_all]
    out_shape = [jax.ShapeDtypeStruct((rows, total), F32), jax.ShapeDtypeStruct((8, blocks * wide), F32)]
    out_specs = [pl.BlockSpec((rows, wide), lambda i, t: (0, at(i, t))), pl.BlockSpec((8, wide), lambda i, t: (0, at(i, t) - first_block))]
    if make:
        in_specs.append(pl.BlockSpec((8, dim), corner))
        args.append(gain8)
        out_shape.insert(0, jax.ShapeDtypeStruct((total, dim), BF16))
        out_specs.insert(0, pl.BlockSpec((wide, dim), lambda i, t: (at(i, t), 0)))
    in_specs.append(ANY)
    args.append(order)
    alias = {len(args) + j: j for j in range(len(prev))}
    return pl.pallas_call(
        body,
        out_shape=out_shape,
        grid_spec=pltpu.PrefetchScalarGridSpec(num_scalar_prefetch=1, grid=(blocks,), in_specs=in_specs + [ANY] * len(prev), out_specs=out_specs),
        input_output_aliases=alias,
        compiler_params=PARAMS,
        name='logits',
    )(*args, *prev)


def grad_rows(z_ref, out_ref, base, col, a, n, meta, rel):
    lse, coef = meta[0:1], meta[1:2]
    wide = meta.shape[1]
    ids = row_ids(wide)
    for r in range(a, a + n, 8):
        prob = jnp.exp(z_ref[pl.ds(r, 8), :] - lse)
        grad = coef * (jnp.where(ids == rel - r, 1.0, 0.0) - prob)
        out_ref[pl.ds(base + r, 8), pl.ds(col, wide)] = grad.astype(BF16)


def dx_call(tab, z_own, z_par, turned_own, turned_par, meta, order, row, first_block, blocks, wide, begin=None):
    rows, _ = z_own.shape
    dim, padded = turned_own.shape
    half = dim // 2
    sub = 256
    keep = begin is not None
    at = lambda i, t: t[row * LIST + i]

    def body(tab_ref, zo_ref, zp_ref, eto_ref, etp_ref, meta_ref, *refs):
        dz_ref, acc_ref = refs[-2:]
        step = pl.program_id(0)
        place = step % 4
        block = first_block + (step // 4) * 8 + place

        @pl.when(tab_ref[ACTIVE + block] > 0)
        def _():
            meta = meta_ref[...]
            tgt = meta[2:3].astype(jnp.int32)
            for h, (z_ref, et_ref) in enumerate(((zo_ref, eto_ref), (zp_ref, etp_ref))):
                dz_ref[pl.ds(h * padded + rows, padded - rows), :] = jnp.zeros((padded - rows, wide), BF16)
                for a in range(0, padded, sub):
                    grad_rows(z_ref, dz_ref, h * padded, 0, a, min(sub, rows - a), meta, tgt - tab_ref[FIRST + h])
                    part = jnp.dot(et_ref[:, pl.ds(a, sub)], dz_ref[pl.ds(h * padded + a, sub), :], preferred_element_type=F32)
                    acc_ref[...] = part if h + a == 0 else acc_ref[...] + part

        @pl.when(tab_ref[ACTIVE + block] == 0)
        def _():
            acc_ref[...] = jnp.zeros_like(acc_ref)

        if not keep:
            refs[1][0] = acc_ref[...]
            return
        start_ref, keep_a, send_a, keep_b, send_b = refs[1:6]
        for q in range(4):

            @pl.when(place == q)
            def _():
                (send_a if q % 2 else keep_a)[0] = acc_ref[pl.ds(0, half), :] + start_ref[0, pl.ds(0, half), :]
                (send_b if q // 2 else keep_b)[q % 2] = acc_ref[pl.ds(half, half), :] + start_ref[0, pl.ds(half, half), :]

    in_specs = [
        pl.BlockSpec((rows, wide), lambda i, t: (0, at(i, t))),
        pl.BlockSpec((rows, wide), lambda i, t: (0, at(i, t))),
        pl.BlockSpec((dim, padded), corner, pipeline_mode=pl.Buffered(1)),
        pl.BlockSpec((dim, padded), corner, pipeline_mode=pl.Buffered(1)),
        pl.BlockSpec((8, wide), lambda i, t: (0, at(i, t))),
        ANY,
    ]
    args = [tab, z_own, z_par, turned_own, turned_par, meta, order]
    one = pl.BlockSpec((1, dim, wide), lambda i, t: (i, 0, 0))
    if keep:
        in_specs.append(one)
        args.append(begin)
        out_shape = [jax.ShapeDtypeStruct((blocks // 2, half, wide), F32)] * 4
        by_place = pl.BlockSpec((1, half, wide), lambda i, t: (i // 2, 0, 0))
        by_chunk = pl.BlockSpec((2, half, wide), lambda i, t: (i // 4, 0, 0))
        out_specs = [by_place, by_place, by_chunk, by_chunk]
    else:
        out_shape = jax.ShapeDtypeStruct((blocks, dim, wide), F32)
        out_specs = one
    return pl.pallas_call(
        body,
        out_shape=out_shape,
        grid_spec=pltpu.PrefetchScalarGridSpec(
            num_scalar_prefetch=1,
            grid=(blocks,),
            in_specs=in_specs,
            out_specs=out_specs,
            scratch_shapes=[pltpu.VMEM((2 * padded, wide), BF16), pltpu.VMEM((dim, wide), F32)],
        ),
        compiler_params=PARAMS,
        name='dx',
    )(*args)


def de_call(tab, which, z, x_all, meta, order, row, part, n_parts, wide, begin=None, into=None):
    rows_all, total = z.shape
    rows = rows_all // n_parts
    dim = x_all.shape[1]
    at = lambda j: (lambda i, t: t[row * LIST + i * SLOTS + j])

    def body(tab_ref, *refs):
        z_refs, x_refs, meta_refs = refs[:SLOTS], refs[SLOTS:2 * SLOTS], refs[2 * SLOTS:3 * SLOTS]
        out_ref, dz_ref, rows_ref = refs[-3:]
        step = pl.program_id(0)

        @pl.when(step == 0)
        def _():
            out_ref[...] = jnp.zeros_like(out_ref) if begin is None else refs[3 * SLOTS + 1][...]

        @pl.when(step * SLOTS < tab_ref[COUNTS + row])
        def _():
            metas, rels = [], []
            for j in range(SLOTS):
                meta = meta_refs[j][...]
                live = jnp.where(step * SLOTS + j < tab_ref[COUNTS + row], 1.0, 0.0)
                rels.append(meta[2:3].astype(jnp.int32) - tab_ref[FIRST + which] - part * rows)
                metas.append(jnp.concatenate([meta[0:1], meta[1:2] * live], axis=0))
                rows_ref[pl.ds(j * wide, wide), :] = x_refs[j][...]
            for a in range(0, rows, PIECE):
                n = min(PIECE, rows - a)
                for j in range(SLOTS):
                    grad_rows(z_refs[j], dz_ref, 0, j * wide, a, n, metas[j], rels[j])
                out_ref[pl.ds(a, n), :] += jnp.dot(dz_ref[pl.ds(a, n), :], rows_ref[...], preferred_element_type=F32)

    maps = [at(j) for j in range(SLOTS)]
    in_specs = [pl.BlockSpec((rows, wide), lambda i, t, m=m: (part, m(i, t))) for m in maps]
    in_specs += [pl.BlockSpec((wide, dim), lambda i, t, m=m: (m(i, t), 0)) for m in maps]
    in_specs += [pl.BlockSpec((8, wide), lambda i, t, m=m: (0, m(i, t))) for m in maps] + [ANY]
    order = meta if order is into else order
    args = [tab] + [z] * SLOTS + [x_all] * SLOTS + [meta] * SLOTS + [order]
    alias = {}
    whole = begin is not None
    if whole:
        in_specs.append(pl.BlockSpec((rows, dim), corner, pipeline_mode=pl.Buffered(1)))
        args.append(begin)
    if into is not None:
        alias = {len(args): 0}
        in_specs.append(ANY)
        args.append(into)
    return pl.pallas_call(
        body,
        out_shape=jax.ShapeDtypeStruct((rows_all if whole else rows, dim), F32),
        grid_spec=pltpu.PrefetchScalarGridSpec(
            num_scalar_prefetch=1,
            grid=(total // wide // SLOTS,),
            in_specs=in_specs,
            out_specs=pl.BlockSpec((rows, dim), lambda i, t: (part if whole else 0, 0)),
            scratch_shapes=[pltpu.VMEM((rows, SLOTS * wide), BF16), pltpu.VMEM((SLOTS * wide, dim), BF16)],
        ),
        input_output_aliases=alias,
        compiler_params=PARAMS,
        name='de',
    )(*args)


def turn_call(emb, order):
    rows, dim = emb.shape
    n = pl.cdiv(rows, 256)

    def body(emb_ref, order_ref, out_ref):
        left = rows - pl.program_id(0) * 256
        row = lax.broadcasted_iota(jnp.int32, emb_ref.shape, 0)
        out_ref[...] = jnp.where(row < left, emb_ref[...], jnp.zeros_like(emb_ref)).T

    return pl.pallas_call(
        body,
        grid=(n,),
        out_shape=jax.ShapeDtypeStruct((dim, n * 256), BF16),
        in_specs=[pl.BlockSpec((256, dim), lambda i: (i, 0)), ANY],
        out_specs=pl.BlockSpec((dim, 256), lambda i: (0, i)),
        compiler_params=PARAMS,
        name='turn',
    )(emb, order)


def flipped(me, mask):
    out = me
    bit = 1
    while bit <= mask:
        if mask & bit:
            out = out + bit - 2 * bit * ((me // bit) % 2)
        bit *= 2
    return out


def share_call(block, shards, ident):
    def body(in_ref, out_ref, send_sem, recv_sem):
        me = lax.axis_index('fsdp')
        peers = [flipped(me, r) for r in range(1, shards)]
        barrier = pltpu.get_barrier_semaphore()
        for peer in peers:
            pl.semaphore_signal(barrier, inc=1, device_id=(peer,), device_id_type=pl.DeviceIdType.MESH)
        pl.semaphore_wait(barrier, shards - 1)
        copies = []
        for r, peer in enumerate(peers):
            copy = pltpu.make_async_remote_copy(src_ref=in_ref, dst_ref=out_ref.at[me], send_sem=send_sem.at[r], recv_sem=recv_sem.at[r], device_id=(peer,), device_id_type=pl.DeviceIdType.MESH)
            copy.start()
            copies.append(copy)
        out_ref[me] = in_ref[...]
        for copy in copies:
            copy.wait()

    return pl.pallas_call(
        body,
        out_shape=jax.ShapeDtypeStruct((shards,) + block.shape, block.dtype),
        in_specs=[pl.BlockSpec(memory_space=pltpu.VMEM)],
        out_specs=pl.BlockSpec(memory_space=pltpu.VMEM),
        scratch_shapes=[pltpu.SemaphoreType.DMA((shards - 1,)), pltpu.SemaphoreType.DMA((shards - 1,))],
        compiler_params=pltpu.CompilerParams(collective_id=ident, has_side_effects=True),
        name='share',
    )(block)


def coef_call(own_stats, par_stats, token, tgt, team, wide, ident):
    tok_dev = token.shape[1]
    n = tok_dev // wide
    n_own, n_par = len(own_stats), len(par_stats)

    def body(*refs):
        own, par = refs[:n_own], refs[n_own:n_own + n_par]
        token_ref, tgt_ref, meta_ref, loss_ref, out_buf, in_buf, send2, back, send_sem, recv_sem, send_sem2, recv_sem2 = refs[n_own + n_par:]
        me = lax.axis_index('fsdp')
        peers = [flipped(me, r) for r in RELATIVE[1:]]
        for ref in (out_buf, send2, meta_ref):
            ref[...] = jnp.zeros_like(ref)
        for k in range(n):
            a = own[k * n_own // n][:, pl.ds(k % (n // n_own) * team * wide, team * wide)]
            b = par[k * n_par // n][:, pl.ds(k % (n // n_par) * team * wide, team * wide)]
            top = jnp.maximum(a[0:1], b[0:1])
            tot = a[1:2] * jnp.exp(a[0:1] - top) + b[1:2] * jnp.exp(b[0:1] - top)
            hit = a[2:3] + b[2:3]
            for p in range(team):
                at = slice(p * wide, (p + 1) * wide)
                dst = out_buf if p else in_buf
                dst[p, 0:1, pl.ds(k * wide, wide)] = top[:, at]
                dst[p, 1:2, pl.ds(k * wide, wide)] = tot[:, at]
                dst[p, 2:3, pl.ds(k * wide, wide)] = hit[:, at]
        barrier = pltpu.get_barrier_semaphore()
        for peer in peers:
            pl.semaphore_signal(barrier, inc=1, device_id=(peer,), device_id_type=pl.DeviceIdType.MESH)
        pl.semaphore_wait(barrier, team - 1)
        copies = []
        for p in range(1, team):
            copy = pltpu.make_async_remote_copy(src_ref=out_buf.at[p], dst_ref=in_buf.at[p], send_sem=send_sem.at[p], recv_sem=recv_sem.at[p], device_id=(peers[p - 1],), device_id_type=pl.DeviceIdType.MESH)
            copy.start()
            copies.append(copy)
        for copy in copies:
            copy.wait()
        top = in_buf[0, 0:1, :]
        for p in range(1, team):
            top = jnp.maximum(top, in_buf[p, 0:1, :])
        tot = jnp.zeros_like(top)
        hit = jnp.zeros_like(top)
        for p in range(team):
            tot = tot + in_buf[p, 1:2, :] * jnp.exp(in_buf[p, 0:1, :] - top)
            hit = hit + in_buf[p, 2:3, :]
        lse = top + jnp.log(tot)
        mask = token_ref[0:1, :]
        tok_loss, d_logp = token_terms(hit - lse, token_ref[1:2, :], token_ref[2:3, :], token_ref[3:4, :])
        send2[0:1, :] = lse
        send2[1:2, :] = jnp.where(mask > 0.0, d_logp / token_ref[4:5, :], 0.0)
        loss_ref[...] = jnp.broadcast_to(jnp.where(mask > 0.0, tok_loss, 0.0), loss_ref.shape)
        copies = []
        for p in range(1, team):
            copy = pltpu.make_async_remote_copy(src_ref=send2, dst_ref=back.at[p], send_sem=send_sem2.at[p], recv_sem=recv_sem2.at[p], device_id=(peers[p - 1],), device_id_type=pl.DeviceIdType.MESH)
            copy.start()
            copies.append(copy)
        back[0] = send2[...]
        for copy in copies:
            copy.wait()
        for k in range(n):
            for p in range(team):
                at = pl.ds((k * team + p) * wide, wide)
                meta_ref[0:2, at] = back[p, 0:2, pl.ds(k * wide, wide)]
        meta_ref[2:3, :] = tgt_ref[0:1, :].astype(F32)

    vmem = pl.BlockSpec(memory_space=pltpu.VMEM)
    return pl.pallas_call(
        body,
        out_shape=[jax.ShapeDtypeStruct((8, n * team * wide), F32), jax.ShapeDtypeStruct((8, tok_dev), F32)],
        in_specs=[vmem] * (n_own + n_par + 2),
        out_specs=[vmem, vmem],
        scratch_shapes=[pltpu.VMEM((team, 8, tok_dev), F32), pltpu.VMEM((team, 8, tok_dev), F32), pltpu.VMEM((8, tok_dev), F32), pltpu.VMEM((team, 8, tok_dev), F32)] + [pltpu.SemaphoreType.DMA((team,))] * 4,
        compiler_params=pltpu.CompilerParams(collective_id=ident, has_side_effects=True),
        name='coef',
    )(*own_stats, *par_stats, token, tgt)


def second_sum(keep_a, recv_a, keep_b, recv_b, order):
    n, half, wide = keep_a.shape

    def body(ka, ra, kb, rb, order_ref, fa, sa, fb, sb):
        fa[0] = ka[0] + ra[0]
        sa[0] = ka[1] + ra[1]
        fb[0] = kb[0] + rb[0]
        sb[0] = kb[1] + rb[1]

    step = half // 2
    two = pl.BlockSpec((2, step, wide), lambda g, i: (g, i, 0))
    one = pl.BlockSpec((1, step, wide), lambda g, i: (g, i, 0))
    return pl.pallas_call(
        body,
        grid=(n // 2, 2),
        out_shape=[jax.ShapeDtypeStruct((n // 2, half, wide), F32)] * 4,
        in_specs=[two] * 4 + [ANY],
        out_specs=[one] * 4,
        compiler_params=PARAMS,
        name='second_sum',
    )(keep_a, recv_a, keep_b, recv_b, order)


def hidden_kernel(fa_ref, ra_ref, fb_ref, rb_ref, hid_ref, gain_ref, dg_ref):
    d_x = jnp.concatenate([(fa_ref[0] + ra_ref[0]).T, (fb_ref[0] + rb_ref[0]).T], axis=1)
    hid = hid_ref[...].astype(F32)
    inv = lax.rsqrt(jnp.mean(hid * hid, axis=-1, keepdims=True) + EPSILON)
    normed = hid * inv
    dg_ref[...] = jnp.broadcast_to(jnp.sum(d_x * normed, axis=0, keepdims=True), dg_ref.shape)
    d_normed = d_x * gain_ref[0:1, :]
    return (inv * (d_normed - normed * jnp.mean(d_normed * normed, axis=-1, keepdims=True))).astype(BF16)


def hidden_call(parts, hidden, gain8, to_spot, prev, order, k):
    n, half, wide = parts[0].shape
    tokens, dim = hidden.shape

    def body(*refs):
        spot_ref, dh_ref, dg_ref, acc_ref = refs[6], *refs[-3:]
        step = pl.program_id(0)
        rows = hidden_kernel(*refs[:6], dg_ref)
        back = lax.dot_general(spot_ref[...], rows, (((0,), (0,)), ((), ())), preferred_element_type=F32)

        @pl.when(step == 0)
        def _():
            acc_ref[...] = back if prev is None else back + refs[-4][...].astype(F32)

        @pl.when(step > 0)
        def _():
            dh_ref[...] = (acc_ref[...] + back).astype(BF16)

    in_specs = [pl.BlockSpec((1, half, wide), lambda i: (i, 0, 0))] * 4 + [
        pl.BlockSpec((wide, dim), lambda i: (k * n + i, 0)),
        pl.BlockSpec((8, dim), corner),
        pl.BlockSpec((wide, tokens), lambda i: (k * n + i, 0)),
        ANY,
    ]
    args = [*parts, hidden, gain8, to_spot, order]
    if prev is not None:
        in_specs.append(pl.BlockSpec((tokens, dim), corner))
        args.append(prev)
    return pl.pallas_call(
        body,
        grid=(n,),
        out_shape=[jax.ShapeDtypeStruct(hidden.shape, BF16), jax.ShapeDtypeStruct((8 * n, dim), F32)],
        in_specs=in_specs,
        out_specs=[pl.BlockSpec((tokens, dim), corner), pl.BlockSpec((8, dim), lambda i: (i, 0))],
        scratch_shapes=[pltpu.VMEM((tokens, dim), F32)],
        compiler_params=PARAMS,
        name='hidden',
    )(*args)


PLAN = (
    ('de_par', 0), ('dx_send', 0), ('dx_send', 1), ('dx_keep', 0), ('de_par', 1), ('dx_keep', 1),
    ('sum_two', 0), ('de_own', 0), ('de_last', 1), ('sum_two', 1), ('finish', 0), ('add', 1), ('finish', 1),
)


def block_lists():
    span = lambda a, n: list(range(a, a + n))
    team = len(RELATIVE)
    halves = lambda b: [sum((span((g * GROUP + k) * team + b, team // 2) for k in range(GROUP)), []) for g in range(CHUNKS // GROUP)]
    lists = [span(k * team, team) for k in range(CHUNKS)]
    lists += [span(g * GROUP * team, GROUP * team) for g in range(CHUNKS // GROUP)]
    return lists + [span(0, CHUNKS * team)] + halves(team // 2) + halves(0)


def solution(mesh):
    shards = mesh.shape['fsdp']
    team = shards // 2
    teams = [list(range(team)), list(range(team, shards))]

    def local(hidden, targets, resp_mask, resp_id, old_logp, ref_logp, rewards, prompt_id, norm_w, embedding):
        tok_dev, dim = hidden.shape
        rows = embedding.shape[0]
        prompts = rewards.shape[0] * shards // GROUP_SIZE
        resp = rewards.shape[0]
        me = lax.axis_index('fsdp')
        wide = tok_dev // CHUNKS
        total = team * tok_dev

        def trade(value, bit):
            return lax.ppermute(value, 'fsdp', [(i, i ^ bit) for i in range(shards)])

        mask_f = resp_mask.astype(F32)
        spots = jnp.arange(tok_dev, dtype=jnp.int32)
        before = jnp.cumsum(resp_mask)
        spot = jnp.where(resp_mask > 0, before - 1, before[-1] + spots - before)
        to_spot = (spots[:, None] == spot[None, :]).astype(BF16)
        rows_first = jnp.dot(to_spot, hidden, preferred_element_type=F32).astype(BF16)
        hid_chunks = [lax.all_gather(rows_first[k * wide:(k + 1) * wide], 'fsdp', axis_index_groups=teams, tiled=True) for k in range(CHUNKS)]

        raw = jnp.stack([targets.astype(F32), mask_f, old_logp, ref_logp, resp_id.astype(F32)])
        raw = lax.dot_general(raw, to_spot.astype(F32), BOTH_LAST, precision=lax.Precision.HIGHEST)
        lanes = lambda v: jnp.pad(v, (0, -v.size % 128)).reshape(-1, 128)
        few = jnp.concatenate([rewards, prompt_id.astype(F32), jnp.sum(mask_f)[None]])
        small = jnp.concatenate([lanes(raw[0]), lanes(few), lanes(norm_w.astype(F32))])
        small = jnp.pad(small, ((0, -small.shape[0] % 8), (0, 0)))
        every = share_call(small, shards, 1)
        emb_later, every = lax.optimization_barrier((embedding, every))
        emb_par = trade(emb_later, team)
        tgt_rows = tok_dev // 128
        rew_all = every[:, tgt_rows, :resp].reshape(-1)
        prompt_all = every[:, tgt_rows, resp:2 * resp].reshape(-1).astype(jnp.int32)
        counts = every[:, tgt_rows, 2 * resp]
        count = jnp.sum(counts)
        gain = every[:, tgt_rows + 1, :norm_w.shape[0]].reshape(-1)
        in_all = (prompt_all[None, :] == jnp.arange(prompts, dtype=jnp.int32)[:, None]).astype(F32)
        totals = jnp.sum(in_all[None] * jnp.stack([rew_all, rew_all * rew_all, jnp.ones_like(rew_all)])[:, None, :], axis=2)
        mean_r = totals[0] / totals[2]
        std_r = jnp.sqrt(jnp.maximum(totals[1] / totals[2] - mean_r * mean_r, 0.0))
        in_own = (prompt_id[None, :] == jnp.arange(prompts, dtype=jnp.int32)[:, None]).astype(F32)
        pick = lambda v: jnp.sum(in_own * v[:, None], axis=0)
        adv_resp = (rewards - pick(mean_r)) / (pick(std_r) + EPSILON)
        adv_tok = jnp.sum(jnp.where(raw[4][None, :] == jnp.arange(resp, dtype=F32)[:, None], adv_resp[:, None], 0.0), axis=0)
        token = jnp.stack([raw[1], raw[2], raw[3], adv_tok, jnp.full_like(mask_f, count)])
        token = jnp.concatenate([token, jnp.zeros((3, tok_dev), F32)])

        in_team = me % team
        place = jnp.bitwise_xor(in_team, jnp.array(RELATIVE, jnp.int32)).astype(jnp.int32)
        tgt_all = every[me - in_team + place, :tgt_rows, :].reshape(team, CHUNKS, wide).transpose(1, 0, 2).reshape(1, total)
        tgt8 = jnp.broadcast_to(tgt_all.astype(jnp.int32), (8, total))
        gain8 = jnp.broadcast_to(gain[None, :], (8, dim))

        active = (counts[me - in_team + place][None, :] > wide * jnp.arange(CHUNKS, dtype=F32)[:, None]).reshape(-1)
        lists = block_lists()
        ids = jnp.array([ids + [0] * (LIST - len(ids)) for ids in lists], jnp.int32)
        used = jnp.array([[1] * len(ids) + [0] * (LIST - len(ids)) for ids in lists], jnp.int32)
        every_id = jnp.arange(LIST, dtype=jnp.int32)
        live = used * jnp.sum((ids[:, :, None] == every_id) * active[None, None, :].astype(jnp.int32), axis=2)
        upto = jnp.sum(live[:, None, :] * (every_id[None, :] <= every_id[:, None]), axis=2)
        n_live = jnp.sum(live, axis=1)
        packed = jnp.minimum(every_id[None, :], n_live[:, None] - 1)
        want = jnp.where(every_id[:N_LISTS, None] < N_LISTS - 4, packed, jnp.maximum(upto - 1, 0))
        chosen = jnp.sum(ids[:, None, :] * live[:, None, :] * (upto[:, None, :] - 1 == want[:, :, None]), axis=2)
        chosen = jnp.where(n_live[:, None] == 0, ids[:, :1], chosen)
        firsts = jnp.stack([me, (me + team) % shards]) * rows
        tab = jnp.concatenate([chosen.reshape(-1), active.astype(jnp.int32), n_live, place, firsts]).astype(jnp.int32)

        stat_own, stat_par, prev, prev_par = [], [], [], []
        order = turned_own = turn_call(embedding, gain8)

        def own(k):
            x_all, z_own, stat = logits_call(tab, 0, embedding, None, tgt8, prev, order, k, k * team, team, wide, hid_chunks[k], gain8)
            prev[:] = [x_all, z_own]
            stat_own.append(stat)
            return stat

        def par(g):
            z, stat = logits_call(tab, 1, emb_par, prev[0], tgt8, prev_par, order, CHUNKS + g, g * GROUP * team, GROUP * team, wide)
            prev_par[:] = [z]
            stat_par.append(stat)
            return stat

        for k in range(CHUNKS - 1):
            order = own(k)
        order = turned_par = turn_call(emb_par, order)
        order = par(0)
        order = own(CHUNKS - 1)
        order = par(1)
        x_all, z_own = prev
        z_par = prev_par[0]
        meta, loss_own = coef_call(stat_own, stat_par, token, tgt8, team, wide, 2)

        state = {}
        order = meta

        def dx_send(k):
            first_block = k * GROUP * team + team // 2
            out = dx_call(tab, z_own, z_par, turned_own, turned_par, meta, order, N_LISTS - 4 + k, first_block, GROUP * team // 2, wide)
            state[k] = trade(out, 1)
            return out

        def dx_keep(k):
            outs = dx_call(tab, z_own, z_par, turned_own, turned_par, meta, order, N_LISTS - 2 + k, k * GROUP * team, GROUP * team // 2, wide, state[k])
            keep_a, send_a, keep_b, send_b = outs
            state[k] = (keep_a, trade(send_a, 2), keep_b, trade(send_b, 4))
            return keep_a

        def sum_two(k):
            fa, sa, fb, sb = second_sum(*state[k], order)
            state[k] = (fa, trade(sa, 4), fb, trade(sb, 2))
            return fa

        def finish(k):
            out, part = hidden_call(state[k], rows_first, gain8, to_spot, state.get('dh'), order, k)
            state['dh'] = out
            state['dg'] = state.get('dg', []) + [part]
            return part

        def de_par(p):
            out = de_call(tab, 1, z_par, x_all, meta, order, CHUNKS + GROUP, p, GROUP, wide)
            state['ship', p] = trade(out, team)
            return out

        def de_own(p):
            state['de'] = de_call(tab, 0, z_own, x_all, meta, order, CHUNKS + GROUP, p, GROUP, wide, state['ship', p], state.get('de'))
            return state['de']

        def de_last(p):
            state['last'] = de_call(tab, 0, z_own, x_all, meta, order, CHUNKS + GROUP, p, GROUP, wide)
            return state['last']

        def add(p):
            more, _ = lax.optimization_barrier((state['ship', p], order))
            state['de'] = state['de'].at[rows // GROUP:].set(state['last'] + more)
            return state['de']

        steps = {'de_last': de_last, 'add': add, 'de_par': de_par, 'dx_send': dx_send, 'dx_keep': dx_keep, 'sum_two': sum_two, 'de_own': de_own, 'finish': finish}
        for name, arg in PLAN:
            order = steps[name](arg)
        d_hidden = state['dh']
        d_embedding = state['de']
        gain_sum = jnp.sum(jnp.concatenate(state['dg'], axis=0)[::8], axis=0)
        last = jnp.concatenate([gain_sum.reshape(-1, 128), lanes(jnp.sum(loss_own[0])[None])])
        last = jnp.pad(last, ((0, -last.shape[0] % 8), (0, 0)))
        last = jnp.sum(share_call(last, shards, 3), axis=0)
        d_norm_w = lax.dynamic_slice(last.reshape(-1), (me * norm_w.shape[0],), (norm_w.shape[0],))
        mean_loss = last[dim // 128, 0] / count
        return mean_loss, d_hidden, d_embedding, d_norm_w

    tok_spec = P('fsdp')
    row_spec = P('fsdp', None)
    return jax.shard_map(local, mesh=mesh, in_specs=(row_spec, tok_spec, tok_spec, tok_spec, tok_spec, tok_spec, tok_spec, tok_spec, tok_spec, row_spec), out_specs=(P(), row_spec, row_spec, tok_spec), check_vma=False)
```
